512 devices in a mesh: energy: 64 (over y, z), block: 4 (over x), role: 2 (over core).
Axes of the slice: x: 4, y: 8, z: 8, core: 2. Of those that a mesh axis runs over, the one named last changes fastest.
Arguments:
- sigma_in: float32 [2, 128, 4, 128, 128], P(None, ('energy', 'role'), 'block'), may hold values from -0.009 to 0.009
- hamiltonian: float32 [4, 128, 128], P('block'), may hold values from -0.5 to 0.5
- coupling: float32 [4, 128, 128], P('block'), may hold values from -0.25 to 0.25
- coulomb: float32 [4, 16384], P('block', ('energy', 'role')), may hold values from 0.2 to 1
- pattern: int32 [2, 4, 4, 4], P(None, 'block'), may hold values 0 or 1
- offsets: int32 [16], replicated, may hold values from 0 to 63
Outputs:
- green: float32 [2, 128, 4, 128, 128], P(None, ('energy', 'role'), 'block')
- sigma_out: float32 [2, 128, 4, 128, 128], P(None, ('energy', 'role'), 'block')
The draws below stay inside these ranges and needn't reach their ends.
All inputs are finite; a program needn't handle non-finite values. No bound on the sum of `pattern` on one device may be relied on, other than what follows from the above.
Results may differ from the reference program's by a relative error of at most 0.0003.
Values sent between devices are 32-bit elements; how exact they have to be, the bound alone decides.
A program may use at most 64 MiB of HBM per device.

```python
import jax
import jax.numpy as jnp
from jax import lax

M = 128
TILE = 32
NW = 16
NB = 4
NE = 128
TL = 4


def place_ends(values, stream_key, smallest, top_value):
    dims = values.shape
    index_at = [jax.random.randint(jax.random.fold_in(stream_key, axis), (), 0, dims[axis]) for axis in range(len(dims))]
    values = values.at[tuple(index_at)].set(smallest)
    longest = dims.index(max(dims))
    index_at[longest] = (index_at[longest] + 1) % dims[longest]
    return values.at[tuple(index_at)].set(top_value)


def steps_of(rng, dims, split, low, largest):
    level, own = 1.0, jax.random.fold_in(rng, 6)
    for position, parts in split:
        heights = jnp.exp(jax.random.uniform(jax.random.fold_in(own, position), (parts,), jnp.float32, low / len(split), largest / len(split)))
        level = level * jnp.repeat(heights, dims[position] // parts).reshape([-1 if axis == position else 1 for axis in range(len(dims))])
    return level


def bell_draw(own_key, extent, scale, limit, shards=(), held_as=jnp.bfloat16):
    values = scale * jax.random.normal(own_key, extent, jnp.float32)
    if shards:
        values = values * steps_of(own_key, extent, shards, -0.22, 0.18)
    return jnp.clip(values, -limit, limit).astype(held_as)


def setup_inputs(seed: int = 0) -> dict:
    seeds = jax.random.split(jax.random.key(seed), 7)
    sigma_in = bell_draw(seeds[0], (2, NE, NB, M, M), 0.0015, 0.009, ((1, 128), (2, 4)), jnp.float32)
    hamiltonian = bell_draw(seeds[1], (NB, M, M), M ** -0.5, 0.5, ((0, 4),), jnp.float32)
    coupling = bell_draw(seeds[2], (NB, M, M), (4 * M) ** -0.5, 0.25, ((0, 4),), jnp.float32)
    coulomb = jnp.clip(0.2 + 0.8 * jax.random.uniform(seeds[3], (NB, M * M), jnp.float32) ** steps_of(seeds[3], (NB, M * M), ((0, 4), (1, 128)), -0.2, 0.2), 0.2, 1.0)
    pattern = place_ends((jax.random.randint(seeds[4], (2, NB, TL, TL), 0, 4) < 3).astype(jnp.int32), jax.random.fold_in(seeds[4], 1), 0, 1)
    offsets = place_ends(jax.random.randint(seeds[5], (NW,), 0, NE // 2), jax.random.fold_in(seeds[5], 1), 0, (NE // 2) - 1).astype(jnp.int32)
    return {"sigma_in": sigma_in, "hamiltonian": hamiltonian, "coupling": coupling, "coulomb": coulomb, "pattern": pattern, "offsets": offsets}


ETA = 0.1
CONTACT = 0.5
HIGH = lax.Precision.HIGHEST

def real_product(left_part, right_part):
    return jnp.einsum('...ij,...jk->...ik', left_part.astype(jnp.float32), right_part.astype(jnp.float32), precision=HIGH, preferred_element_type=jnp.float32)

def complex_dot(first, second):
    rr = real_product(first[0], second[0]) - real_product(first[1], second[1])
    ri = real_product(first[0], second[1]) + real_product(first[1], second[0])
    return jnp.stack([rr, ri])

def real_left(matrix, value):
    return jnp.einsum('ij,...jk->...ik', matrix.astype(jnp.float32), value.astype(jnp.float32), precision=HIGH, preferred_element_type=jnp.float32)

def real_right(value, matrix):
    return jnp.einsum('...ij,jk->...ik', value.astype(jnp.float32), matrix.astype(jnp.float32), precision=HIGH, preferred_element_type=jnp.float32)

def expand(tiles):
    count = tiles.shape[-1]
    lead = tiles.shape[:-2]
    big = jnp.broadcast_to(tiles[..., :, None, :, None], lead + (count, TILE, count, TILE))
    return big.reshape(lead + (count * TILE, count * TILE)).astype(jnp.float32)

def symmetric(block):
    return 0.5 * (block + jnp.swapaxes(block, -1, -2))

def system_matrix(energy, onsite_block, sigma_block, identity):
    real_part = energy[:, None, None] * identity - onsite_block - sigma_block[0]
    imag_part = ETA * identity - sigma_block[1]
    return jnp.stack([real_part, imag_part])

def contact(system, coupling_block, ends):
    square_coupling = jnp.dot(coupling_block.T.astype(jnp.float32), coupling_block.astype(jnp.float32), precision=HIGH, preferred_element_type=jnp.float32)
    return jnp.stack([system[0], system[1] + ends * CONTACT * square_coupling])

def invert(system):
    width = system.shape[-1]
    a_part = system[0]
    b_part = system[1]
    a_trans = jnp.swapaxes(a_part, -1, -2)
    b_trans = jnp.swapaxes(b_part, -1, -2)
    p_part = real_product(a_trans, a_part) + real_product(b_trans, b_part)
    q_part = real_product(a_trans, b_part) - real_product(b_trans, a_part)
    upper_rows = jnp.concatenate([p_part, -q_part], axis=-1)
    lower_rows = jnp.concatenate([q_part, p_part], axis=-1)
    normal = jnp.concatenate([upper_rows, lower_rows], axis=-2)
    factor = jnp.linalg.cholesky(normal)
    stacked = jnp.concatenate([a_trans, -b_trans], axis=-2)
    middle = jax.scipy.linalg.solve_triangular(factor, stacked, lower=True)
    solved = jax.scipy.linalg.solve_triangular(factor, middle, lower=True, trans=1)
    return jnp.stack([solved[..., :width, :], solved[..., width:, :]])

def project(coupling_block, left_green):
    return real_right(real_left(coupling_block.T, left_green), coupling_block)

def backstep(left_green, coupling_block, right_full):
    first = real_right(left_green, coupling_block)
    second = complex_dot(first, right_full)
    third = real_right(second, coupling_block.T)
    return left_green + complex_dot(third, left_green)

def screen(values, offsets):
    energies = values.shape[1]
    factor = 6.0 / energies / (2.0 * 3.141592653589793)
    widths = ((0, 0), (energies, 0)) + ((0, 0),) * (values.ndim - 2)
    padded = jnp.pad(values, widths)

    def one_offset(offset_index, total):
        start = (energies - offsets[offset_index]).astype(jnp.int32)
        moved = lax.dynamic_slice_in_dim(padded, start, energies, 1)
        pol_real = factor * jnp.sum(values[0] * moved[0] - values[1] * moved[1], axis=0)
        pol_imag = factor * jnp.sum(values[0] * moved[1] + values[1] * moved[0], axis=0)
        self_real = moved[0] * pol_real - moved[1] * pol_imag
        self_imag = moved[0] * pol_imag + moved[1] * pol_real
        return total + jnp.stack([self_real, self_imag])
    summed = lax.fori_loop(0, offsets.shape[0], one_offset, jnp.zeros_like(values))
    return summed / offsets.shape[0]

def reference(sigma_in, hamiltonian, coupling, coulomb, pattern, offsets):
    identity = jnp.eye(M, dtype=jnp.float32)
    masks = expand(pattern)
    energy = -3.0 + 6.0 * jnp.arange(NE).astype(jnp.float32) / NE
    lefts = []
    sent = None
    for block_index in range(NB):
        onsite = symmetric(hamiltonian[block_index] * masks[0, block_index])
        system = system_matrix(energy, onsite, sigma_in[:, :, block_index], identity)
        if block_index == NB - 1:
            system = contact(system, coupling[block_index], 1.0)
        if block_index > 0:
            system = system - sent
        left_green = invert(system)
        lefts.append(left_green)
        if block_index < NB - 1:
            sent = project(coupling[block_index], left_green)
    full = lefts[-1]
    fulls = [full]
    for block_index in range(NB - 2, -1, -1):
        full = backstep(lefts[block_index], coupling[block_index], full)
        fulls.insert(0, full)
    green = jnp.stack(fulls, axis=2)
    outgoing = []
    for block_index in range(NB):
        summed = screen(green[:, :, block_index], offsets)
        effective = coulomb[block_index].reshape(M, M) * masks[1, block_index]
        outgoing.append(summed * (effective * effective))
    return (green, jnp.stack(outgoing, axis=2))
```

```python
import functools

import jax
import jax.numpy as jnp
from jax import lax
from jax.experimental import pallas as pl
from jax.experimental.pallas import tpu as pltpu
from jax.sharding import PartitionSpec as P

TILE = 32
ETA = 0.1
CONTACT = 0.5
HIGH = lax.Precision.HIGHEST
F32 = jnp.float32


def dot(a, b):
    return jnp.dot(a, b, precision=HIGH, preferred_element_type=F32)


def row_of(x, k):
    return jnp.broadcast_to(x[k : k + 1, :], (8, 128))


def column_of(x, k):
    return jnp.broadcast_to(x[:, k : k + 1], (8, 128))


def small_inverse(cols):
    row = lax.broadcasted_iota(jnp.int32, (8, 128), 0)
    for k in range(8):
        here = row == k
        pr, pi = row_of(cols[k][0], k), row_of(cols[k][1], k)
        r = 1.0 / (pr * pr + pi * pi)
        ir, ii = pr * r, -(pi * r)
        cr, ci = cols[k]
        tr = jnp.where(here, -ir, cr * ir - ci * ii)
        ti = jnp.where(here, -ii, cr * ii + ci * ir)
        new = []
        for j in range(8):
            if j == k:
                new.append((-tr, -ti))
                continue
            a, b = cols[j]
            ar, ai = row_of(a, k), row_of(b, k)
            za, zb = jnp.where(here, 0.0, a), jnp.where(here, 0.0, b)
            new.append((za - (tr * ar - ti * ai), zb - (tr * ai + ti * ar)))
        cols = new
    return cols


def panel_inverse(pr, pi, base):
    lane = lax.broadcasted_iota(jnp.int32, (8, 128), 1)
    row = lax.broadcasted_iota(jnp.int32, (8, 128), 0)
    for q in range(4):
        at = base + 8 * q
        inv = small_inverse([(column_of(pr[q], at + j), column_of(pi[q], at + j)) for j in range(8)])
        inside = (lane >= at) & (lane < at + 8)
        sr = jnp.where(inside, jnp.where(lane - at == row, 1.0, 0.0), pr[q])
        si = jnp.where(inside, 0.0, pi[q])
        nr = ni = None
        for j in range(8):
            a, b = row_of(sr, j), row_of(si, j)
            er, ei = inv[j]
            xr, xi = er * a - ei * b, er * b + ei * a
            nr, ni = (xr, xi) if nr is None else (nr + xr, ni + xi)
        rows = [(row_of(nr, j), row_of(ni, j)) for j in range(8)]
        for i in range(4):
            if i == q:
                continue
            ar, ai = jnp.where(inside, 0.0, pr[i]), jnp.where(inside, 0.0, pi[i])
            for j in range(8):
                cr, ci = column_of(pr[i], at + j), column_of(pi[i], at + j)
                ar = ar - (cr * rows[j][0] - ci * rows[j][1])
                ai = ai - (cr * rows[j][1] + ci * rows[j][0])
            pr[i], pi[i] = ar, ai
        pr[q], pi[q] = nr, ni
    return pr, pi


def inverses(matrices):
    lane = lax.broadcasted_iota(jnp.int32, (96, 128), 1)
    state = [[[part[32 * s : 32 * s + 32] for s in range(4)] for part in m] for m in matrices]
    for p in range(4):
        base = 32 * p
        others = [(p + 1) % 4, (p + 2) % 4, (p + 3) % 4]
        panels = []
        for xr, xi in state:
            a = [xr[p][8 * i : 8 * i + 8] for i in range(4)]
            b = [xi[p][8 * i : 8 * i + 8] for i in range(4)]
            a, b = panel_inverse(a, b, base)
            panels.append((jnp.concatenate(a, 0), jnp.concatenate(b, 0)))
        following = []
        for (xr, xi), (nr, ni) in zip(state, panels):
            old_r = jnp.concatenate([xr[o] for o in others], 0)
            old_i = jnp.concatenate([xi[o] for o in others], 0)
            left = jnp.concatenate([old_r[:, base : base + 32], old_i[:, base : base + 32]], 1)
            right = jnp.concatenate([jnp.concatenate([nr, ni], 1), jnp.concatenate([-ni, nr], 1)], 0)
            change = dot(left, right)
            inside = (lane >= base) & (lane < base + 32)
            new_r = jnp.where(inside, 0.0, old_r) - change[:, :128]
            new_i = jnp.where(inside, 0.0, old_i) - change[:, 128:]
            yr, yi = [None] * 4, [None] * 4
            for t, o in enumerate(others):
                yr[o], yi[o] = new_r[32 * t : 32 * t + 32], new_i[32 * t : 32 * t + 32]
            yr[p], yi[p] = nr, ni
            following.append((yr, yi))
        state = following
    return [(jnp.concatenate(a, 0), jnp.concatenate(b, 0)) for a, b in state]


def complex_dot(a, b):
    left = jnp.concatenate(a, 1)
    right = jnp.concatenate([jnp.concatenate([b[0], b[1]], 1), jnp.concatenate([-b[1], b[0]], 1)], 0)
    whole = dot(left, right)
    return whole[:, :128], whole[:, 128:]


def real_left(k, g):
    whole = dot(k, jnp.concatenate(g, 1))
    return whole[:, :128], whole[:, 128:]


def real_right(g, k):
    whole = dot(jnp.concatenate(g, 0), k)
    return whole[:128], whole[128:]


def minus(a, b):
    return a[0] - b[0], a[1] - b[1]


def solve_kernel(x_ref, o_ref):
    position = lax.axis_index("block")
    forward = position >= 2
    first = jnp.where(forward, 0, 3)
    second = jnp.where(forward, 1, 2)
    third = jnp.where(forward, 2, 1)
    fourth = jnp.where(forward, 3, 0)
    near = jnp.where(forward, 0, 2)
    far = jnp.where(forward, 2, 0)

    def both(index, plain):
        k = x_ref[index, 2]
        kt = k.T
        return jnp.where(plain, k, kt), jnp.where(plain, kt, k)

    k1, k1t = both(near, forward)
    k2, k2t = both(1, forward)
    k3, k3t = both(far, jnp.logical_not(forward))
    ga, gd = inverses([(x_ref[first, 0], x_ref[first, 1]), (x_ref[fourth, 0], x_ref[fourth, 1])])
    sb = minus((x_ref[second, 0], x_ref[second, 1]), real_right(real_left(k1t, ga), k1))
    (gb,) = inverses([sb])
    gd_k3 = real_right(gd, k3)
    k3t_gd = real_left(k3t, gd)
    sc = minus((x_ref[third, 0], x_ref[third, 1]), real_right(k3t_gd, k3))
    sc = minus(sc, real_right(real_left(k2t, gb), k2))
    (gc,) = inverses([sc])
    back = complex_dot(complex_dot(gd_k3, gc), k3t_gd)
    inner = (position == 1) | (position == 2)
    o_ref[0] = jnp.where(inner, gc[0], gd[0] + back[0])
    o_ref[1] = jnp.where(inner, gc[1], gd[1] + back[1])


def screen_kernel(energies, count, offsets_ref, v_ref, weight_ref, o_ref, padded, polar):
    padded[:, :energies] = jnp.zeros((2, energies, 128), F32)
    padded[:, energies:] = v_ref[...]
    factor = 6.0 / energies / (2.0 * 3.141592653589793)

    def polarize(w, carry):
        start = energies - offsets_ref[w]
        mr, mi = padded[0, pl.ds(start, energies), :], padded[1, pl.ds(start, energies), :]
        vr, vi = v_ref[0], v_ref[1]
        polar[0, pl.ds(w, 1), :] = factor * jnp.sum(vr * mr - vi * mi, axis=0, keepdims=True)
        polar[1, pl.ds(w, 1), :] = factor * jnp.sum(vr * mi + vi * mr, axis=0, keepdims=True)
        return carry

    lax.fori_loop(0, count, polarize, 0)
    weight = weight_ref[...]
    scale = weight * weight * (1.0 / count)
    rows = 64
    for n in range(0, energies, rows):

        def interact(w, total):
            start = energies - offsets_ref[w] + n
            mr, mi = padded[0, pl.ds(start, rows), :], padded[1, pl.ds(start, rows), :]
            pr, pi = polar[0, pl.ds(w, 1), :], polar[1, pl.ds(w, 1), :]
            return total[0] + (mr * pr - mi * pi), total[1] + (mr * pi + mi * pr)

        zero = jnp.zeros((rows, 128), F32)
        tr, ti = lax.fori_loop(0, count, interact, (zero, zero))
        o_ref[0, n : n + rows] = tr * scale
        o_ref[1, n : n + rows] = ti * scale


def in_vmem():
    return pl.BlockSpec(memory_space=pltpu.VMEM)


def expand(tiles):
    big = jnp.broadcast_to(tiles[:, None, :, None], (tiles.shape[0], TILE, tiles.shape[1], TILE))
    return big.reshape(tiles.shape[0] * TILE, tiles.shape[1] * TILE).astype(F32)


def body(sigma_in, hamiltonian, coupling, coulomb, pattern, offsets):
    width = hamiltonian.shape[-1]
    position = lax.axis_index("block")
    blocks = lax.axis_size("block")
    groups = lax.axis_size("energy") * lax.axis_size("role")
    place = lax.axis_index("energy") * lax.axis_size("role") + lax.axis_index("role")
    identity = jnp.eye(width, dtype=F32)
    energy = -3.0 + 6.0 * place.astype(F32) / groups
    onsite = hamiltonian[0] * expand(pattern[0, 0])
    onsite = 0.5 * (onsite + onsite.T)
    k = coupling[0]
    ends = jnp.where(position == blocks - 1, 1.0, 0.0)
    square = jnp.dot(k.T, k, precision=HIGH, preferred_element_type=F32)
    real = energy * identity - onsite - sigma_in[0, 0, 0]
    imag = ETA * identity - sigma_in[1, 0, 0] + ends * CONTACT * square
    mine = jnp.stack([real, imag, k])
    every = lax.all_to_all(jnp.broadcast_to(mine[None], (blocks, *mine.shape)), "block", 0, 0, tiled=True)
    green = pl.pallas_call(
        solve_kernel,
        out_shape=jax.ShapeDtypeStruct((2, width, width), F32),
        in_specs=[in_vmem()],
        out_specs=in_vmem(),
        cost_estimate=pl.CostEstimate(flops=2_000_000_000, bytes_accessed=900_000, transcendentals=0),
    )(every)
    values = lax.all_to_all(green, ("energy", "role"), split_axis=1, concat_axis=1, tiled=True)
    tiles = lax.dynamic_slice_in_dim(pattern[1, 0], place // TILE, 1, 0)
    weight = coulomb * jnp.repeat(tiles, TILE, axis=1).astype(F32)
    elements = pl.pallas_call(
        functools.partial(screen_kernel, groups, offsets.shape[0]),
        out_shape=jax.ShapeDtypeStruct((2, groups, width), F32),
        in_specs=[pl.BlockSpec(memory_space=pltpu.SMEM), in_vmem(), in_vmem()],
        out_specs=in_vmem(),
        scratch_shapes=[pltpu.VMEM((2, 2 * groups, width), F32), pltpu.VMEM((2, offsets.shape[0], width), F32)],
    )(offsets, values, weight)
    returned = lax.all_to_all(elements, ("energy", "role"), split_axis=1, concat_axis=1, tiled=True)
    return green[:, None, None], returned[:, None, None]


def solution(mesh):
    spread = P(None, ("energy", "role"), "block", None, None)
    in_specs = (
        spread,
        P("block", None, None),
        P("block", None, None),
        P("block", ("energy", "role")),
        P(None, "block", None, None),
        P(),
    )
    return jax.shard_map(body, mesh=mesh, in_specs=in_specs, out_specs=(spread, spread), check_vma=False)
```

```python
import functools

import jax
import jax.numpy as jnp
from jax import lax
from jax.experimental import pallas as pl
from jax.experimental.pallas import tpu as pltpu
from jax.sharding import PartitionSpec as P

TILE = 32
ETA = 0.1
CONTACT = 0.5
HIGH = lax.Precision.HIGHEST
F32 = jnp.float32


def dot(a, b):
    return jnp.dot(a, b, precision=HIGH, preferred_element_type=F32)


def row_of(x, k):
    return jnp.broadcast_to(x[k : k + 1, :], (8, 128))


def column_of(x, k):
    return jnp.broadcast_to(x[:, k : k + 1], (8, 128))


def small_inverse(cols):
    row = lax.broadcasted_iota(jnp.int32, (8, 128), 0)
    for k in range(8):
        here = row == k
        pr, pi = row_of(cols[k][0], k), row_of(cols[k][1], k)
        r = 1.0 / (pr * pr + pi * pi)
        ir, ii = pr * r, -(pi * r)
        cr, ci = cols[k]
        tr = jnp.where(here, -ir, cr * ir - ci * ii)
        ti = jnp.where(here, -ii, cr * ii + ci * ir)
        new = []
        for j in range(8):
            if j == k:
                new.append((-tr, -ti))
                continue
            a, b = cols[j]
            ar, ai = row_of(a, k), row_of(b, k)
            za, zb = jnp.where(here, 0.0, a), jnp.where(here, 0.0, b)
            new.append((za - (tr * ar - ti * ai), zb - (tr * ai + ti * ar)))
        cols = new
    return cols


def panel_inverse(pr, pi, base):
    lane = lax.broadcasted_iota(jnp.int32, (8, 128), 1)
    row = lax.broadcasted_iota(jnp.int32, (8, 128), 0)
    for q in range(4):
        at = base + 8 * q
        inv = small_inverse([(column_of(pr[q], at + j), column_of(pi[q], at + j)) for j in range(8)])
        inside = (lane >= at) & (lane < at + 8)
        sr = jnp.where(inside, jnp.where(lane - at == row, 1.0, 0.0), pr[q])
        si = jnp.where(inside, 0.0, pi[q])
        nr = ni = None
        for j in range(8):
            a, b = row_of(sr, j), row_of(si, j)
            er, ei = inv[j]
            xr, xi = er * a - ei * b, er * b + ei * a
            nr, ni = (xr, xi) if nr is None else (nr + xr, ni + xi)
        rows = [(row_of(nr, j), row_of(ni, j)) for j in range(8)]
        for i in range(4):
            if i == q:
                continue
            ar, ai = jnp.where(inside, 0.0, pr[i]), jnp.where(inside, 0.0, pi[i])
            for j in range(8):
                cr, ci = column_of(pr[i], at + j), column_of(pi[i], at + j)
                ar = ar - (cr * rows[j][0] - ci * rows[j][1])
                ai = ai - (cr * rows[j][1] + ci * rows[j][0])
            pr[i], pi[i] = ar, ai
        pr[q], pi[q] = nr, ni
    return pr, pi


def inverses(matrices):
    lane = lax.broadcasted_iota(jnp.int32, (96, 128), 1)
    state = [[[part[32 * s : 32 * s + 32] for s in range(4)] for part in m] for m in matrices]
    for p in range(4):
        base = 32 * p
        others = [(p + 1) % 4, (p + 2) % 4, (p + 3) % 4]
        panels = []
        for xr, xi in state:
            a = [xr[p][8 * i : 8 * i + 8] for i in range(4)]
            b = [xi[p][8 * i : 8 * i + 8] for i in range(4)]
            a, b = panel_inverse(a, b, base)
            panels.append((jnp.concatenate(a, 0), jnp.concatenate(b, 0)))
        following = []
        for (xr, xi), (nr, ni) in zip(state, panels):
            old_r = jnp.concatenate([xr[o] for o in others], 0)
            old_i = jnp.concatenate([xi[o] for o in others], 0)
            left = jnp.concatenate([old_r[:, base : base + 32], old_i[:, base : base + 32]], 1)
            right = jnp.concatenate([jnp.concatenate([nr, ni], 1), jnp.concatenate([-ni, nr], 1)], 0)
            change = dot(left, right)
            inside = (lane >= base) & (lane < base + 32)
            new_r = jnp.where(inside, 0.0, old_r) - change[:, :128]
            new_i = jnp.where(inside, 0.0, old_i) - change[:, 128:]
            yr, yi = [None] * 4, [None] * 4
            for t, o in enumerate(others):
                yr[o], yi[o] = new_r[32 * t : 32 * t + 32], new_i[32 * t : 32 * t + 32]
            yr[p], yi[p] = nr, ni
            following.append((yr, yi))
        state = following
    return [(jnp.concatenate(a, 0), jnp.concatenate(b, 0)) for a, b in state]


def complex_dot(a, b):
    left = jnp.concatenate(a, 1)
    right = jnp.concatenate([jnp.concatenate([b[0], b[1]], 1), jnp.concatenate([-b[1], b[0]], 1)], 0)
    whole = dot(left, right)
    return whole[:, :128], whole[:, 128:]


def real_left(k, g):
    whole = dot(k, jnp.concatenate(g, 1))
    return whole[:, :128], whole[:, 128:]


def real_right(g, k):
    whole = dot(jnp.concatenate(g, 0), k)
    return whole[:128], whole[128:]


def minus(a, b):
    return a[0] - b[0], a[1] - b[1]


def solve_kernel(x_ref, o_ref):
    position = lax.axis_index("block")
    forward = position >= 2
    first = jnp.where(forward, 0, 3)
    second = jnp.where(forward, 1, 2)
    third = jnp.where(forward, 2, 1)
    fourth = jnp.where(forward, 3, 0)
    near = jnp.where(forward, 0, 2)
    far = jnp.where(forward, 2, 0)

    def both(index, plain):
        k = x_ref[index, 2]
        kt = k.T
        return jnp.where(plain, k, kt), jnp.where(plain, kt, k)

    k1, k1t = both(near, forward)
    k2, k2t = both(1, forward)
    k3, k3t = both(far, jnp.logical_not(forward))
    ga, gd = inverses([(x_ref[first, 0], x_ref[first, 1]), (x_ref[fourth, 0], x_ref[fourth, 1])])
    sb = minus((x_ref[second, 0], x_ref[second, 1]), real_right(real_left(k1t, ga), k1))
    (gb,) = inverses([sb])
    gd_k3 = real_right(gd, k3)
    k3t_gd = real_left(k3t, gd)
    sc = minus((x_ref[third, 0], x_ref[third, 1]), real_right(k3t_gd, k3))
    sc = minus(sc, real_right(real_left(k2t, gb), k2))
    (gc,) = inverses([sc])
    back = complex_dot(complex_dot(gd_k3, gc), k3t_gd)
    inner = (position == 1) | (position == 2)
    o_ref[0] = jnp.where(inner, gc[0], gd[0] + back[0])
    o_ref[1] = jnp.where(inner, gc[1], gd[1] + back[1])


def tile_row(tiles_ref, p, i, rows, width):
    lane = lax.broadcasted_iota(jnp.int32, (rows, width), 1)
    strip = jnp.zeros((rows, width), F32)
    for j in range(width // TILE):
        strip = jnp.where((lane >= TILE * j) & (lane < TILE * j + TILE), tiles_ref[p, 0, i, j].astype(F32), strip)
    return strip


def exchange(place, cur, mid, out, send, recv, base):
    slow, fast, row_partner, slow_partner = place
    started = []

    def push(source, target, index, device):
        copy = pltpu.make_async_remote_copy(
            src_ref=source,
            dst_ref=target,
            send_sem=send.at[base + index],
            recv_sem=recv.at[base + index],
            device_id=device,
            device_id_type=pl.DeviceIdType.MESH,
        )
        copy.start()
        return copy

    fasts = sorted(range(1, 16), key=lambda s: -min(s, 16 - s))
    slows = sorted(range(1, 8), key=lambda s: -min(s, 8 - s))
    one, two = [], []
    for s in fasts:
        t, device = row_partner(s)
        one.append(push(cur.at[0, :, t, :], mid.at[0, :, fast, :], s, device))
    for s in slows:
        t, device = slow_partner(s)
        two.append(push(cur.at[1, t], mid.at[1, slow], 16 + s, device))
    mid[0, :, pl.ds(fast, 1), :] = cur[0, :, pl.ds(fast, 1), :]
    mid[1, pl.ds(slow, 1)] = cur[1, pl.ds(slow, 1)]
    for copy in two:
        copy.wait()
    for s in fasts:
        t, device = row_partner(s)
        started.append(push(mid.at[1, :, t, :], out.at[1, :, fast, :], 24 + s, device))
    for copy in one:
        copy.wait()
    for s in slows:
        t, device = slow_partner(s)
        started.append(push(mid.at[0, t], out.at[0, slow], 40 + s, device))
    out[1, :, pl.ds(fast, 1), :] = mid[1, :, pl.ds(fast, 1), :]
    out[0, pl.ds(slow, 1)] = mid[0, pl.ds(slow, 1)]
    for copy in started:
        copy.wait()


def screen_kernel(count, offsets_ref, tiles_ref, v_ref, coulomb_ref, o_ref, mid, padded, polar, done, mid_back, send, recv):
    energies = 128
    factor = 6.0 / energies / (2.0 * 3.141592653589793)
    e, c = lax.axis_index("energy"), lax.axis_index("role")
    slow, z = e // 8, lax.rem(e, 8)
    fast = 2 * z + c

    def row_partner(s):
        t = lax.rem(fast + s, 16)
        return t, {"energy": slow * 8 + t // 2, "role": lax.rem(t, 2)}

    def slow_partner(s):
        t = lax.rem(slow + s, 8)
        return t, {"energy": t * 8 + z, "role": c}

    place = slow, fast, row_partner, slow_partner
    barrier = pltpu.get_barrier_semaphore()
    for partner, others in ((row_partner, 16), (slow_partner, 8)):
        for s in range(1, others):
            pl.semaphore_signal(barrier, inc=1, device_id=partner(s)[1], device_id_type=pl.DeviceIdType.MESH)
    padded[:, :8] = jnp.zeros((2, 8, 16, 128), F32)
    pl.semaphore_wait(barrier, 22)
    exchange(place, v_ref, mid, padded.at[:, 8:], send, recv, 0)
    flat = padded.reshape(2, 2 * energies, 128)
    result = done.reshape(2, energies, 128)

    def polarize(w, carry):
        start = energies - offsets_ref[w]
        mr, mi = flat[0, pl.ds(start, energies), :], flat[1, pl.ds(start, energies), :]
        vr, vi = flat[0, energies:, :], flat[1, energies:, :]
        polar[0, pl.ds(w, 1), :] = factor * jnp.sum(vr * mr - vi * mi, axis=0, keepdims=True)
        polar[1, pl.ds(w, 1), :] = factor * jnp.sum(vr * mi + vi * mr, axis=0, keepdims=True)
        return carry

    lax.fori_loop(0, count, polarize, 0)
    weight = coulomb_ref[...] * tile_row(tiles_ref, 1, (2 * e + c) // TILE, 1, 128)
    scale = weight * weight * (1.0 / count)
    rows = 64
    for n in range(0, energies, rows):

        def interact(w, total):
            start = energies - offsets_ref[w] + n
            mr, mi = flat[0, pl.ds(start, rows), :], flat[1, pl.ds(start, rows), :]
            pr, pi = polar[0, pl.ds(w, 1), :], polar[1, pl.ds(w, 1), :]
            return total[0] + (mr * pr - mi * pi), total[1] + (mr * pi + mi * pr)

        zero = jnp.zeros((rows, 128), F32)
        tr, ti = lax.fori_loop(0, count, interact, (zero, zero))
        result[0, n : n + rows] = tr * scale
        result[1, n : n + rows] = ti * scale
    exchange(place, done, mid_back, o_ref, send, recv, 48)


def system_kernel(tiles_ref, sigma_ref, hamiltonian_ref, coupling_ref, o_ref):
    position = lax.axis_index("block")
    place = lax.axis_index("energy") * lax.axis_size("role") + lax.axis_index("role")
    width = hamiltonian_ref.shape[-1]
    row = lax.broadcasted_iota(jnp.int32, (width, width), 0)
    column = lax.broadcasted_iota(jnp.int32, (width, width), 1)
    strips = [tile_row(tiles_ref, 0, i, TILE, width) for i in range(width // TILE)]
    masked = hamiltonian_ref[0] * jnp.concatenate(strips, 0)
    onsite = 0.5 * (masked + masked.T)
    groups = lax.axis_size("energy") * lax.axis_size("role")
    energy = -3.0 + 6.0 * place.astype(F32) / groups
    k = coupling_ref[0]
    diagonal = row == column
    o_ref[0] = jnp.where(diagonal, energy, 0.0) - onsite - sigma_ref[0, 0, 0]
    bare = jnp.where(diagonal, ETA, 0.0) - sigma_ref[1, 0, 0]
    last = position == lax.axis_size("block") - 1
    o_ref[1] = bare + jnp.where(last, CONTACT * dot(k.T, k), 0.0)
    o_ref[2] = k


def in_vmem():
    return pl.BlockSpec(memory_space=pltpu.VMEM)


def in_smem():
    return pl.BlockSpec(memory_space=pltpu.SMEM)


def body(sigma_in, hamiltonian, coupling, coulomb, pattern, offsets):
    width = hamiltonian.shape[-1]
    blocks = lax.axis_size("block")
    count = offsets.shape[0]
    mine = pl.pallas_call(
        system_kernel,
        out_shape=jax.ShapeDtypeStruct((3, width, width), F32),
        in_specs=[in_smem(), in_vmem(), in_vmem(), in_vmem()],
        out_specs=in_vmem(),
    )(pattern, sigma_in, hamiltonian, coupling)
    every = lax.all_to_all(jnp.broadcast_to(mine[None], (blocks, *mine.shape)), "block", 0, 0, tiled=True)
    green = pl.pallas_call(
        solve_kernel,
        out_shape=jax.ShapeDtypeStruct((2, width, width), F32),
        in_specs=[in_vmem()],
        out_specs=in_vmem(),
        cost_estimate=pl.CostEstimate(flops=2_000_000_000, bytes_accessed=900_000, transcendentals=0),
    )(every)
    planes = (2, 8, 16, width)
    screened = pl.pallas_call(
        functools.partial(screen_kernel, count),
        out_shape=jax.ShapeDtypeStruct(planes, F32),
        in_specs=[in_smem(), in_smem(), in_vmem(), in_vmem()],
        out_specs=in_vmem(),
        scratch_shapes=[
            pltpu.VMEM(planes, F32),
            pltpu.VMEM((2, 16, 16, width), F32),
            pltpu.VMEM((2, count, width), F32),
            pltpu.VMEM(planes, F32),
            pltpu.VMEM(planes, F32),
            pltpu.SemaphoreType.DMA((96,)),
            pltpu.SemaphoreType.DMA((96,)),
        ],
        compiler_params=pltpu.CompilerParams(collective_id=1, has_side_effects=True),
    )(offsets, pattern, green.reshape(planes), coulomb)
    spread = (2, 1, 1, width, width)
    return green.reshape(spread), screened.reshape(spread)


def solution(mesh):
    spread = P(None, ("energy", "role"), "block", None, None)
    in_specs = (
        spread,
        P("block", None, None),
        P("block", None, None),
        P("block", ("energy", "role")),
        P(None, "block", None, None),
        P(),
    )
    return jax.shard_map(body, mesh=mesh, in_specs=in_specs, out_specs=(spread, spread), check_vma=False)
```

```python
import functools

import jax
import jax.numpy as jnp
from jax import lax
from jax.experimental import pallas as pl
from jax.experimental.pallas import tpu as pltpu
from jax.sharding import PartitionSpec as P

TILE = 32
ETA = 0.1
CONTACT = 0.5
HIGH = lax.Precision.HIGHEST
F32 = jnp.float32


def dot(a, b):
    return jnp.dot(a, b, precision=HIGH, preferred_element_type=F32)


def row_of(x, k):
    return jnp.broadcast_to(x[k : k + 1, :], (8, 128))


def column_of(x, k):
    return jnp.broadcast_to(x[:, k : k + 1], (8, 128))


def times(a, b):
    return a[0] * b[0] - a[1] * b[1], a[0] * b[1] + a[1] * b[0]


def pair_step(cols, panel, k):
    row = lax.broadcasted_iota(jnp.int32, (8, 128), 0)
    l = k + 1
    at_k, at_l = row == k, row == l
    both = at_k | at_l
    ck, cl = cols[k], cols[l]
    a = row_of(ck[0], k), row_of(ck[1], k)
    b = row_of(cl[0], k), row_of(cl[1], k)
    c = row_of(ck[0], l), row_of(ck[1], l)
    d = row_of(cl[0], l), row_of(cl[1], l)
    ad, bc = times(a, d), times(b, c)
    er, ei = ad[0] - bc[0], ad[1] - bc[1]
    r = 1.0 / (er * er + ei * ei)
    kd, lc = times(ck, d), times(cl, c)
    la, kb = times(cl, a), times(ck, b)
    uk = tuple(jnp.where(at_k, -d[p], jnp.where(at_l, c[p], kd[p] - lc[p])) for p in (0, 1))
    ul = tuple(jnp.where(at_k, b[p], jnp.where(at_l, -a[p], la[p] - kb[p])) for p in (0, 1))
    inv = er * r, -(ei * r)
    tk, tl = times(uk, inv), times(ul, inv)

    def update(z):
        x, y = z
        u = times(tk, (row_of(x, k), row_of(y, k)))
        v = times(tl, (row_of(x, l), row_of(y, l)))
        return jnp.where(both, 0.0, x) - (u[0] + v[0]), jnp.where(both, 0.0, y) - (u[1] + v[1])

    return [z if j <= l else update(z) for j, z in enumerate(cols)], update(panel)


def panels_inverse(chains, base):
    lane = lax.broadcasted_iota(jnp.int32, (8, 128), 1)
    row = lax.broadcasted_iota(jnp.int32, (8, 128), 0)
    chains = [(list(a), list(b)) for a, b in chains]
    total = len(chains[0][0])
    for q in range(4):
        at = base + 8 * q
        inside = (lane >= at) & (lane < at + 8)
        unit = jnp.where(lane - at == row, 1.0, 0.0)
        work = []
        for pr, pi in chains:
            cols = [(column_of(pr[q], at + j), column_of(pi[q], at + j)) for j in range(8)]
            work.append((cols, (jnp.where(inside, unit, pr[q]), jnp.where(inside, 0.0, pi[q]))))
        for k in range(0, 8, 2):
            work = [pair_step(cols, panel, k) for cols, panel in work]
        rows = [[(row_of(n[0], j), row_of(n[1], j)) for j in range(8)] for _, n in work]
        for i in [(q + 1 + i) % total for i in range(total)]:
            if i == q:
                continue
            for (pr, pi), own in zip(chains, rows):
                terms = [times((column_of(pr[i], at + j), column_of(pi[i], at + j)), own[j]) for j in range(8)]
                while len(terms) > 1:
                    pairs = zip(terms[::2], terms[1::2])
                    terms = [(m[0] + n[0], m[1] + n[1]) for m, n in pairs]
                pr[i] = jnp.where(inside, 0.0, pr[i]) - terms[0][0]
                pi[i] = jnp.where(inside, 0.0, pi[i]) - terms[0][1]
        for (pr, pi), (_, n) in zip(chains, work):
            pr[q], pi[q] = n
    return chains


def inverses(matrices):
    lane = lax.broadcasted_iota(jnp.int32, (8, 128), 1)
    state = [[[part[8 * s : 8 * s + 8] for s in range(16)] for part in m] for m in matrices]
    for p in range(4):
        base = 32 * p
        own = [4 * p + i for i in range(4 if p == 3 else 5)]
        others = [s % 16 for s in range(4 * p + len(own), 4 * p + 16)]
        inside = (lane >= base) & (lane < base + 32)
        panels = panels_inverse([([xr[s] for s in own], [xi[s] for s in own]) for xr, xi in state], base)
        following = []
        for (xr, xi), (nr, ni) in zip(state, panels):
            old_r = jnp.concatenate([xr[o] for o in others], 0)
            old_i = jnp.concatenate([xi[o] for o in others], 0)
            left = jnp.concatenate([old_r[:, base : base + 32], old_i[:, base : base + 32]], 1)
            fr, fi = jnp.concatenate(nr[:4], 0), jnp.concatenate(ni[:4], 0)
            right = jnp.concatenate([jnp.concatenate([fr, fi], 1), jnp.concatenate([-fi, fr], 1)], 0)
            change = dot(left, right)
            yr, yi = [None] * 16, [None] * 16
            for t, o in enumerate(others):
                yr[o] = jnp.where(inside, 0.0, xr[o]) - change[8 * t : 8 * t + 8, :128]
                yi[o] = jnp.where(inside, 0.0, xi[o]) - change[8 * t : 8 * t + 8, 128:]
            for t, o in enumerate(own):
                yr[o], yi[o] = nr[t], ni[t]
            following.append((yr, yi))
        state = following
    return [(jnp.concatenate(a, 0), jnp.concatenate(b, 0)) for a, b in state]


def complex_dot(a, b):
    left = jnp.concatenate(a, 1)
    right = jnp.concatenate([jnp.concatenate([b[0], b[1]], 1), jnp.concatenate([-b[1], b[0]], 1)], 0)
    whole = dot(left, right)
    return whole[:, :128], whole[:, 128:]


def real_left(k, g):
    whole = dot(k, jnp.concatenate(g, 1))
    return whole[:, :128], whole[:, 128:]


def real_right(g, k):
    whole = dot(jnp.concatenate(g, 0), k)
    return whole[:128], whole[128:]


def minus(a, b):
    return a[0] - b[0], a[1] - b[1]


def solve_kernel(x_ref, o_ref, again_ref):
    position = lax.axis_index("block")
    forward = position >= 2
    first = jnp.where(forward, 0, 3)
    second = jnp.where(forward, 1, 2)
    third = jnp.where(forward, 2, 1)
    fourth = jnp.where(forward, 3, 0)
    near = jnp.where(forward, 0, 2)
    far = jnp.where(forward, 2, 0)

    def both(index, plain):
        k = x_ref[index, 2]
        kt = k.T
        return jnp.where(plain, k, kt), jnp.where(plain, kt, k)

    k1, k1t = both(near, forward)
    k2, k2t = both(1, forward)
    k3, k3t = both(far, jnp.logical_not(forward))
    ga, gd = inverses([(x_ref[first, 0], x_ref[first, 1]), (x_ref[fourth, 0], x_ref[fourth, 1])])
    sb = minus((x_ref[second, 0], x_ref[second, 1]), real_right(real_left(k1t, ga), k1))
    (gb,) = inverses([sb])
    gd_k3 = real_right(gd, k3)
    k3t_gd = real_left(k3t, gd)
    sc = minus((x_ref[third, 0], x_ref[third, 1]), real_right(k3t_gd, k3))
    sc = minus(sc, real_right(real_left(k2t, gb), k2))
    (gc,) = inverses([sc])
    back = complex_dot(complex_dot(gd_k3, gc), k3t_gd)
    inner = (position == 1) | (position == 2)
    for part in (0, 1):
        value = jnp.where(inner, gc[part], gd[part] + back[part])
        o_ref[part] = value
        again_ref[part] = value


def tile_row(tiles_ref, p, i, rows, width):
    lane = lax.broadcasted_iota(jnp.int32, (rows, width), 1)
    strip = jnp.zeros((rows, width), F32)
    for j in range(width // TILE):
        strip = jnp.where((lane >= TILE * j) & (lane < TILE * j + TILE), tiles_ref[p, 0, i, j].astype(F32), strip)
    return strip


def exchange(place, cur, mid, out, send, recv, base):
    slow, fast, row_partner, slow_partner = place
    started = []

    def push(source, target, index, device):
        copy = pltpu.make_async_remote_copy(
            src_ref=source,
            dst_ref=target,
            send_sem=send.at[base + index],
            recv_sem=recv.at[base + index],
            device_id=device,
            device_id_type=pl.DeviceIdType.MESH,
        )
        copy.start()
        return copy

    fasts = sorted(range(1, 16), key=lambda s: -min(s, 16 - s))
    slows = sorted(range(1, 8), key=lambda s: -min(s, 8 - s))
    one, two = [], []
    for s in fasts:
        t, device = row_partner(s)
        one.append(push(cur.at[0, :, t, :], mid.at[0, :, fast, :], s, device))
    for s in slows:
        t, device = slow_partner(s)
        two.append(push(cur.at[1, t], mid.at[1, slow], 16 + s, device))
    mid[0, :, pl.ds(fast, 1), :] = cur[0, :, pl.ds(fast, 1), :]
    mid[1, pl.ds(slow, 1)] = cur[1, pl.ds(slow, 1)]
    for copy in two:
        copy.wait()
    for s in fasts:
        t, device = row_partner(s)
        started.append(push(mid.at[1, :, t, :], out.at[1, :, fast, :], 24 + s, device))
    for copy in one:
        copy.wait()
    for s in slows:
        t, device = slow_partner(s)
        started.append(push(mid.at[0, t], out.at[0, slow], 40 + s, device))
    out[1, :, pl.ds(fast, 1), :] = mid[1, :, pl.ds(fast, 1), :]
    out[0, pl.ds(slow, 1)] = mid[0, pl.ds(slow, 1)]
    for copy in started:
        copy.wait()


def screen_kernel(count, offsets_ref, tiles_ref, v_ref, coulomb_ref, o_ref, mid, padded, polar, done, mid_back, send, recv):
    energies = 128
    factor = 6.0 / energies / (2.0 * 3.141592653589793)
    e, c = lax.axis_index("energy"), lax.axis_index("role")
    slow, z = e // 8, lax.rem(e, 8)
    fast = 2 * z + c

    def row_partner(s):
        t = lax.rem(fast + s, 16)
        return t, {"energy": slow * 8 + t // 2, "role": lax.rem(t, 2)}

    def slow_partner(s):
        t = lax.rem(slow + s, 8)
        return t, {"energy": t * 8 + z, "role": c}

    place = slow, fast, row_partner, slow_partner
    barrier = pltpu.get_barrier_semaphore()
    for partner, others in ((row_partner, 16), (slow_partner, 8)):
        for s in range(1, others):
            pl.semaphore_signal(barrier, inc=1, device_id=partner(s)[1], device_id_type=pl.DeviceIdType.MESH)
    padded[:, :8] = jnp.zeros((2, 8, 16, 128), F32)
    pl.semaphore_wait(barrier, 22)
    exchange(place, v_ref, mid, padded.at[:, 8:], send, recv, 0)
    flat = padded.reshape(2, 2 * energies, 128)
    result = done.reshape(2, energies, 128)

    def polarize(w, carry):
        start = energies - offsets_ref[w]
        mr, mi = flat[0, pl.ds(start, energies), :], flat[1, pl.ds(start, energies), :]
        vr, vi = flat[0, energies:, :], flat[1, energies:, :]
        polar[0, pl.ds(w, 1), :] = factor * jnp.sum(vr * mr - vi * mi, axis=0, keepdims=True)
        polar[1, pl.ds(w, 1), :] = factor * jnp.sum(vr * mi + vi * mr, axis=0, keepdims=True)
        return carry

    lax.fori_loop(0, count, polarize, 0)
    weight = coulomb_ref[...] * tile_row(tiles_ref, 1, (2 * e + c) // TILE, 1, 128)
    scale = weight * weight * (1.0 / count)
    rows = 64
    for n in range(0, energies, rows):

        def interact(w, total):
            start = energies - offsets_ref[w] + n
            mr, mi = flat[0, pl.ds(start, rows), :], flat[1, pl.ds(start, rows), :]
            pr, pi = polar[0, pl.ds(w, 1), :], polar[1, pl.ds(w, 1), :]
            return total[0] + (mr * pr - mi * pi), total[1] + (mr * pi + mi * pr)

        zero = jnp.zeros((rows, 128), F32)
        tr, ti = lax.fori_loop(0, count, interact, (zero, zero))
        result[0, n : n + rows] = tr * scale
        result[1, n : n + rows] = ti * scale
    exchange(place, done, mid_back, o_ref, send, recv, 48)


def gather_kernel(tiles, sigma, hamiltonian, coupling, o_ref, tiles_ref, sigma_ref, hamiltonian_ref, coupling_ref, local, send, recv):
    count = 4
    position = lax.axis_index("block")
    right, left = lax.rem(position + 1, count), lax.rem(position + count - 1, count)
    barrier = pltpu.get_barrier_semaphore()
    for neighbour in (left, right):
        pl.semaphore_signal(barrier, inc=1, device_id={"block": neighbour}, device_id_type=pl.DeviceIdType.MESH)
    pairs = (tiles, tiles_ref), (sigma, sigma_ref), (hamiltonian, hamiltonian_ref), (coupling, coupling_ref)
    loads = [pltpu.make_async_copy(source, target, local.at[i]) for i, (source, target) in enumerate(pairs)]
    for load in loads:
        load.start()
    for load in loads:
        load.wait()
    place = lax.axis_index("energy") * lax.axis_size("role") + lax.axis_index("role")
    width = hamiltonian_ref.shape[-1]
    row = lax.broadcasted_iota(jnp.int32, (width, width), 0)
    column = lax.broadcasted_iota(jnp.int32, (width, width), 1)
    strips = [tile_row(tiles_ref, 0, i, TILE, width) for i in range(width // TILE)]
    masked = hamiltonian_ref[0] * jnp.concatenate(strips, 0)
    onsite = 0.5 * (masked + masked.T)
    groups = lax.axis_size("energy") * lax.axis_size("role")
    energy = -3.0 + 6.0 * place.astype(F32) / groups
    k = coupling_ref[0]
    diagonal = row == column
    real = jnp.where(diagonal, energy, 0.0) - onsite - sigma_ref[0, 0, 0]
    bare = jnp.where(diagonal, ETA, 0.0) - sigma_ref[1, 0, 0]
    last = position == count - 1
    o_ref[pl.ds(position, 1)] = jnp.stack([real, bare + jnp.where(last, CONTACT * dot(k.T, k), 0.0), k])[None]
    pl.semaphore_wait(barrier, 2)
    half = width // 2
    upper, lower = pl.ds(0, half), pl.ds(half, half)

    def push(owner, rows, index, device):
        return pltpu.make_async_remote_copy(
            src_ref=o_ref.at[owner, :, rows, :],
            dst_ref=o_ref.at[owner, :, rows, :],
            send_sem=send.at[index],
            recv_sem=recv.at[index],
            device_id={"block": device},
            device_id_type=pl.DeviceIdType.MESH,
        )

    first = [push(position, upper, 0, right), push(position, lower, 1, left)]
    second = [push(position, lower, 2, right), push(position, upper, 3, left)]
    for copy in first + second:
        copy.start()
    onward = [push(left, upper, 4, right), push(right, lower, 5, left)]
    for copy, following in zip(first, onward):
        copy.wait_recv()
        following.start()
    for copy in first:
        copy.wait_send()
    for copy in second + onward:
        copy.wait()


def in_vmem():
    return pl.BlockSpec(memory_space=pltpu.VMEM)


def in_smem():
    return pl.BlockSpec(memory_space=pltpu.SMEM)


def body(sigma_in, hamiltonian, coupling, coulomb, pattern, offsets):
    width = hamiltonian.shape[-1]
    count = offsets.shape[0]
    every = pl.pallas_call(
        gather_kernel,
        out_shape=jax.ShapeDtypeStruct((4, 3, width, width), F32),
        in_specs=[pl.BlockSpec(memory_space=pl.ANY)] * 4,
        out_specs=in_vmem(),
        scratch_shapes=[
            pltpu.SMEM(pattern.shape, pattern.dtype),
            pltpu.VMEM(sigma_in.shape, F32),
            pltpu.VMEM(hamiltonian.shape, F32),
            pltpu.VMEM(coupling.shape, F32),
            pltpu.SemaphoreType.DMA((4,)),
            pltpu.SemaphoreType.DMA((6,)),
            pltpu.SemaphoreType.DMA((6,)),
        ],
        compiler_params=pltpu.CompilerParams(collective_id=2, has_side_effects=True, vmem_limit_bytes=66_180_000),
    )(pattern, sigma_in, hamiltonian, coupling)
    green, again = pl.pallas_call(
        solve_kernel,
        out_shape=[jax.ShapeDtypeStruct((2, width, width), F32)] * 2,
        in_specs=[in_vmem()],
        out_specs=[in_vmem()] * 2,
        compiler_params=pltpu.CompilerParams(vmem_limit_bytes=24 << 20),
    )(every)
    planes = (2, 8, 16, width)
    screened = pl.pallas_call(
        functools.partial(screen_kernel, count),
        out_shape=jax.ShapeDtypeStruct(planes, F32),
        in_specs=[in_smem(), in_smem(), in_vmem(), in_vmem()],
        out_specs=in_vmem(),
        scratch_shapes=[
            pltpu.VMEM(planes, F32),
            pltpu.VMEM((2, 16, 16, width), F32),
            pltpu.VMEM((2, count, width), F32),
            pltpu.VMEM(planes, F32),
            pltpu.VMEM(planes, F32),
            pltpu.SemaphoreType.DMA((96,)),
            pltpu.SemaphoreType.DMA((96,)),
        ],
        compiler_params=pltpu.CompilerParams(collective_id=1, has_side_effects=True, vmem_limit_bytes=8 << 20),
    )(offsets, pattern, again.reshape(planes), coulomb)
    spread = (2, 1, 1, width, width)
    return green.reshape(spread), screened.reshape(spread)


def solution(mesh):
    spread = P(None, ("energy", "role"), "block", None, None)
    in_specs = (
        spread,
        P("block", None, None),
        P("block", None, None),
        P("block", ("energy", "role")),
        P(None, "block", None, None),
        P(),
    )
    return jax.shard_map(body, mesh=mesh, in_specs=in_specs, out_specs=(spread, spread), check_vma=False)
```

```python
import functools

import jax
import jax.numpy as jnp
from jax import lax
from jax.experimental import pallas as pl
from jax.experimental.pallas import tpu as pltpu
from jax.sharding import PartitionSpec as P

TILE = 32
ETA = 0.1
CONTACT = 0.5
HIGH = lax.Precision.HIGHEST
F32 = jnp.float32


def dot(a, b):
    return jnp.dot(a, b, precision=HIGH, preferred_element_type=F32)


def row_of(x, k):
    return jnp.broadcast_to(x[k : k + 1, :], (8, 128))


def column_of(x, k):
    return jnp.broadcast_to(x[:, k : k + 1], (8, 128))


def times(a, b):
    return a[0] * b[0] - a[1] * b[1], a[0] * b[1] + a[1] * b[0]


def pair_step(cols, panel, k):
    row = lax.broadcasted_iota(jnp.int32, (8, 128), 0)
    l = k + 1
    at_k, at_l = row == k, row == l
    both = at_k | at_l
    ck, cl = cols[k], cols[l]
    a = row_of(ck[0], k), row_of(ck[1], k)
    b = row_of(cl[0], k), row_of(cl[1], k)
    c = row_of(ck[0], l), row_of(ck[1], l)
    d = row_of(cl[0], l), row_of(cl[1], l)
    ad, bc = times(a, d), times(b, c)
    er, ei = ad[0] - bc[0], ad[1] - bc[1]
    r = 1.0 / (er * er + ei * ei)
    kd, lc = times(ck, d), times(cl, c)
    la, kb = times(cl, a), times(ck, b)
    uk = tuple(jnp.where(at_k, -d[p], jnp.where(at_l, c[p], kd[p] - lc[p])) for p in (0, 1))
    ul = tuple(jnp.where(at_k, b[p], jnp.where(at_l, -a[p], la[p] - kb[p])) for p in (0, 1))
    inv = er * r, -(ei * r)
    tk, tl = times(uk, inv), times(ul, inv)

    def update(z):
        x, y = z
        u = times(tk, (row_of(x, k), row_of(y, k)))
        v = times(tl, (row_of(x, l), row_of(y, l)))
        return jnp.where(both, 0.0, x) - (u[0] + v[0]), jnp.where(both, 0.0, y) - (u[1] + v[1])

    return [z if j <= l else update(z) for j, z in enumerate(cols)], update(panel)


def panels_inverse(chains, base):
    lane = lax.broadcasted_iota(jnp.int32, (8, 128), 1)
    row = lax.broadcasted_iota(jnp.int32, (8, 128), 0)
    chains = [(list(a), list(b)) for a, b in chains]
    total = len(chains[0][0])
    for q in range(4):
        at = base + 8 * q
        inside = (lane >= at) & (lane < at + 8)
        unit = jnp.where(lane - at == row, 1.0, 0.0)
        work = []
        for pr, pi in chains:
            cols = [(column_of(pr[q], at + j), column_of(pi[q], at + j)) for j in range(8)]
            work.append((cols, (jnp.where(inside, unit, pr[q]), jnp.where(inside, 0.0, pi[q]))))
        for k in range(0, 8, 2):
            work = [pair_step(cols, panel, k) for cols, panel in work]
        rows = [[(row_of(n[0], j), row_of(n[1], j)) for j in range(8)] for _, n in work]
        for i in [(q + 1 + i) % total for i in range(total)]:
            if i == q:
                continue
            for (pr, pi), own in zip(chains, rows):
                terms = [times((column_of(pr[i], at + j), column_of(pi[i], at + j)), own[j]) for j in range(8)]
                while len(terms) > 1:
                    pairs = zip(terms[::2], terms[1::2])
                    terms = [(m[0] + n[0], m[1] + n[1]) for m, n in pairs]
                pr[i] = jnp.where(inside, 0.0, pr[i]) - terms[0][0]
                pi[i] = jnp.where(inside, 0.0, pi[i]) - terms[0][1]
        for (pr, pi), (_, n) in zip(chains, work):
            pr[q], pi[q] = n
    return chains


def inverses(matrices):
    lane = lax.broadcasted_iota(jnp.int32, (8, 128), 1)
    state = [[[part[8 * s : 8 * s + 8] for s in range(16)] for part in m] for m in matrices]
    for p in range(4):
        base = 32 * p
        own = [4 * p + i for i in range(4 if p == 3 else 5)]
        others = [s % 16 for s in range(4 * p + len(own), 4 * p + 16)]
        inside = (lane >= base) & (lane < base + 32)
        panels = panels_inverse([([xr[s] for s in own], [xi[s] for s in own]) for xr, xi in state], base)
        following = []
        for (xr, xi), (nr, ni) in zip(state, panels):
            old_r = jnp.concatenate([xr[o] for o in others], 0)
            old_i = jnp.concatenate([xi[o] for o in others], 0)
            left = jnp.concatenate([old_r[:, base : base + 32], old_i[:, base : base + 32]], 1)
            fr, fi = jnp.concatenate(nr[:4], 0), jnp.concatenate(ni[:4], 0)
            right = jnp.concatenate([jnp.concatenate([fr, fi], 1), jnp.concatenate([-fi, fr], 1)], 0)
            change = dot(left, right)
            yr, yi = [None] * 16, [None] * 16
            for t, o in enumerate(others):
                yr[o] = jnp.where(inside, 0.0, xr[o]) - change[8 * t : 8 * t + 8, :128]
                yi[o] = jnp.where(inside, 0.0, xi[o]) - change[8 * t : 8 * t + 8, 128:]
            for t, o in enumerate(own):
                yr[o], yi[o] = nr[t], ni[t]
            following.append((yr, yi))
        state = following
    return [(jnp.concatenate(a, 0), jnp.concatenate(b, 0)) for a, b in state]


def complex_dot(a, b):
    left = jnp.concatenate(a, 1)
    right = jnp.concatenate([jnp.concatenate([b[0], b[1]], 1), jnp.concatenate([-b[1], b[0]], 1)], 0)
    whole = dot(left, right)
    return whole[:, :128], whole[:, 128:]


def real_left(k, g):
    whole = dot(k, jnp.concatenate(g, 1))
    return whole[:, :128], whole[:, 128:]


def real_right(g, k):
    whole = dot(jnp.concatenate(g, 0), k)
    return whole[:128], whole[128:]


def minus(a, b):
    return a[0] - b[0], a[1] - b[1]


def tile_row(tiles_ref, p, i, rows, width):
    lane = lax.broadcasted_iota(jnp.int32, (rows, width), 1)
    strip = jnp.zeros((rows, width), F32)
    for j in range(width // TILE):
        strip = jnp.where((lane >= TILE * j) & (lane < TILE * j + TILE), tiles_ref[p, 0, i, j].astype(F32), strip)
    return strip


def exchange(place, cur, mid, out, send, recv, base):
    slow, fast, row_partner, slow_partner = place
    started = []

    def push(source, target, index, device):
        copy = pltpu.make_async_remote_copy(
            src_ref=source,
            dst_ref=target,
            send_sem=send.at[base + index],
            recv_sem=recv.at[base + index],
            device_id=device,
            device_id_type=pl.DeviceIdType.MESH,
        )
        copy.start()
        return copy

    fasts = sorted(range(1, 16), key=lambda s: -min(s, 16 - s))
    slows = sorted(range(1, 8), key=lambda s: -min(s, 8 - s))
    one, two = [], []
    for s in fasts:
        t, device = row_partner(s)
        one.append(push(cur.at[0, :, t, :], mid.at[0, :, fast, :], s, device))
    for s in slows:
        t, device = slow_partner(s)
        two.append(push(cur.at[1, t], mid.at[1, slow], 16 + s, device))
    mid[0, :, pl.ds(fast, 1), :] = cur[0, :, pl.ds(fast, 1), :]
    mid[1, pl.ds(slow, 1)] = cur[1, pl.ds(slow, 1)]
    for copy in two:
        copy.wait()
    for s in fasts:
        t, device = row_partner(s)
        started.append(push(mid.at[1, :, t, :], out.at[1, :, fast, :], 24 + s, device))
    for copy in one:
        copy.wait()
    for s in slows:
        t, device = slow_partner(s)
        started.append(push(mid.at[0, t], out.at[0, slow], 40 + s, device))
    out[1, :, pl.ds(fast, 1), :] = mid[1, :, pl.ds(fast, 1), :]
    out[0, pl.ds(slow, 1)] = mid[0, pl.ds(slow, 1)]
    for copy in started:
        copy.wait()


MESH = pl.DeviceIdType.MESH


def build_system(position, tiles_ref, sigma_ref, hamiltonian_ref, coupling_ref, x_ref):
    place = lax.axis_index("energy") * lax.axis_size("role") + lax.axis_index("role")
    width = hamiltonian_ref.shape[-1]
    row = lax.broadcasted_iota(jnp.int32, (width, width), 0)
    column = lax.broadcasted_iota(jnp.int32, (width, width), 1)
    strips = [tile_row(tiles_ref, 0, i, TILE, width) for i in range(width // TILE)]
    masked = hamiltonian_ref[0] * jnp.concatenate(strips, 0)
    onsite = 0.5 * (masked + masked.T)
    groups = lax.axis_size("energy") * lax.axis_size("role")
    energy = -3.0 + 6.0 * place.astype(F32) / groups
    k = coupling_ref[0]
    diagonal = row == column
    real = jnp.where(diagonal, energy, 0.0) - onsite - sigma_ref[0, 0, 0]
    bare = jnp.where(diagonal, ETA, 0.0) - sigma_ref[1, 0, 0]
    imag = bare + jnp.where(position == 3, CONTACT * dot(k.T, k), 0.0)
    x_ref[pl.ds(position, 1)] = jnp.stack([real, imag])[None]


def solve(position, x_ref, k_ref, couplings_arrived):
    forward = position >= 2
    first = jnp.where(forward, 0, 3)
    second = jnp.where(forward, 1, 2)
    third = jnp.where(forward, 2, 1)
    fourth = jnp.where(forward, 3, 0)

    def both(index, plain):
        k = k_ref[index]
        kt = k.T
        return jnp.where(plain, k, kt), jnp.where(plain, kt, k)

    ga, gd = inverses([(x_ref[first, 0], x_ref[first, 1]), (x_ref[fourth, 0], x_ref[fourth, 1])])
    couplings_arrived()
    k1, k1t = both(jnp.where(forward, 0, 2), forward)
    k2, k2t = both(1, forward)
    k3, k3t = both(jnp.where(forward, 2, 0), jnp.logical_not(forward))
    sb = minus((x_ref[second, 0], x_ref[second, 1]), real_right(real_left(k1t, ga), k1))
    (gb,) = inverses([sb])
    gd_k3 = real_right(gd, k3)
    k3t_gd = real_left(k3t, gd)
    sc = minus((x_ref[third, 0], x_ref[third, 1]), real_right(k3t_gd, k3))
    sc = minus(sc, real_right(real_left(k2t, gb), k2))
    (gc,) = inverses([sc])
    back = complex_dot(complex_dot(gd_k3, gc), k3t_gd)
    inner = (position == 1) | (position == 2)
    return [jnp.where(inner, gc[part], gd[part] + back[part]) for part in (0, 1)]


def whole_kernel(
    count,
    offsets_ref,
    tiles,
    sigma,
    hamiltonian,
    coupling,
    coulomb,
    green_ref,
    o_ref,
    tiles_ref,
    sigma_ref,
    hamiltonian_ref,
    coulomb_ref,
    x_ref,
    k_ref,
    held,
    mid,
    padded,
    polar,
    done,
    mid_back,
    local,
    ring_send,
    ring_recv,
    send,
    recv,
):
    energies = 128
    factor = 6.0 / energies / (2.0 * 3.141592653589793)
    position = lax.axis_index("block")
    e, c = lax.axis_index("energy"), lax.axis_index("role")
    slow, z = e // 8, lax.rem(e, 8)
    fast = 2 * z + c
    right, opposite, left = [lax.rem(position + s, 4) for s in (1, 2, 3)]
    pairs = (
        (coupling, k_ref.at[pl.ds(position, 1)]),
        (tiles, tiles_ref),
        (sigma, sigma_ref),
        (hamiltonian, hamiltonian_ref),
        (coulomb, coulomb_ref),
    )
    loads = [pltpu.make_async_copy(source, target, local.at[i]) for i, (source, target) in enumerate(pairs)]
    for load in loads:
        load.start()

    def row_partner(s):
        t = lax.rem(fast + s, 16)
        return t, {"energy": slow * 8 + t // 2, "role": lax.rem(t, 2)}

    def slow_partner(s):
        t = lax.rem(slow + s, 8)
        return t, {"energy": t * 8 + z, "role": c}

    place = slow, fast, row_partner, slow_partner
    barrier = pltpu.get_barrier_semaphore()
    for partner, others in ((row_partner, 16), (slow_partner, 8)):
        for s in range(1, others):
            pl.semaphore_signal(barrier, inc=1, device_id=partner(s)[1], device_id_type=MESH)
    for block in (right, opposite, left):
        pl.semaphore_signal(barrier, inc=1, device_id={"block": block}, device_id_type=MESH)
    padded[:, :8] = jnp.zeros((2, 8, 16, 128), F32)
    for load in loads:
        load.wait()
    build_system(position, tiles_ref, sigma_ref, hamiltonian_ref, k_ref.at[pl.ds(position, 1)], x_ref)
    pl.semaphore_wait(barrier, 25)

    def push(ref, index, block):
        return pltpu.make_async_remote_copy(
            src_ref=ref,
            dst_ref=ref,
            send_sem=ring_send.at[index],
            recv_sem=ring_recv.at[index],
            device_id={"block": block},
            device_id_type=MESH,
        )

    def system(owner, lower):
        return x_ref.at[owner, :, pl.ds(64 * lower, 64), :]

    early = [push(system(position, 0), 0, right), push(system(position, 1), 1, left)]
    late = [push(system(position, 1), 2, right), push(system(position, 0), 3, left)]
    onward = [push(system(left, 0), 4, right), push(system(right, 1), 5, left)]
    couplings = [push(k_ref.at[position], 6 + i, block) for i, block in enumerate((right, opposite, left))]
    for copy in early + late:
        copy.start()
    for copy, following in zip(early, onward):
        copy.wait_recv()
        following.start()
    for copy in couplings:
        copy.start()
    for copy in early:
        copy.wait_send()
    for copy in late + onward:
        copy.wait()

    def couplings_arrived():
        for copy in couplings:
            copy.wait()

    green = solve(position, x_ref, k_ref, couplings_arrived)
    for part in (0, 1):
        held[part] = green[part].reshape(8, 16, 128)
        green_ref[part] = green[part]
    exchange(place, held, mid, padded.at[:, 8:], send, recv, 0)
    flat = padded.reshape(2, 2 * energies, 128)
    result = done.reshape(2, energies, 128)

    def polarize(w, carry):
        start = energies - offsets_ref[w]
        mr, mi = flat[0, pl.ds(start, energies), :], flat[1, pl.ds(start, energies), :]
        vr, vi = flat[0, energies:, :], flat[1, energies:, :]
        polar[0, pl.ds(w, 1), :] = factor * jnp.sum(vr * mr - vi * mi, axis=0, keepdims=True)
        polar[1, pl.ds(w, 1), :] = factor * jnp.sum(vr * mi + vi * mr, axis=0, keepdims=True)
        return carry

    lax.fori_loop(0, count, polarize, 0)
    weight = coulomb_ref[...] * tile_row(tiles_ref, 1, (2 * e + c) // TILE, 1, 128)
    scale = weight * weight * (1.0 / count)
    rows = 64
    for n in range(0, energies, rows):

        def interact(w, total):
            start = energies - offsets_ref[w] + n
            mr, mi = flat[0, pl.ds(start, rows), :], flat[1, pl.ds(start, rows), :]
            pr, pi = polar[0, pl.ds(w, 1), :], polar[1, pl.ds(w, 1), :]
            return total[0] + (mr * pr - mi * pi), total[1] + (mr * pi + mi * pr)

        zero = jnp.zeros((rows, 128), F32)
        tr, ti = lax.fori_loop(0, count, interact, (zero, zero))
        result[0, n : n + rows] = tr * scale
        result[1, n : n + rows] = ti * scale
    exchange(place, done, mid_back, o_ref, send, recv, 48)


def in_vmem():
    return pl.BlockSpec(memory_space=pltpu.VMEM)


def in_smem():
    return pl.BlockSpec(memory_space=pltpu.SMEM)


def body(sigma_in, hamiltonian, coupling, coulomb, pattern, offsets):
    width = hamiltonian.shape[-1]
    count = offsets.shape[0]
    planes = (2, 8, 16, width)
    green, screened = pl.pallas_call(
        functools.partial(whole_kernel, count),
        out_shape=[jax.ShapeDtypeStruct((2, width, width), F32), jax.ShapeDtypeStruct(planes, F32)],
        in_specs=[in_smem()] + [pl.BlockSpec(memory_space=pl.ANY)] * 5,
        out_specs=[in_vmem()] * 2,
        scratch_shapes=[
            pltpu.SMEM(pattern.shape, pattern.dtype),
            pltpu.VMEM(sigma_in.shape, F32),
            pltpu.VMEM(hamiltonian.shape, F32),
            pltpu.VMEM(coulomb.shape, F32),
            pltpu.VMEM((4, 2, width, width), F32),
            pltpu.VMEM((4, width, width), F32),
            pltpu.VMEM(planes, F32),
            pltpu.VMEM(planes, F32),
            pltpu.VMEM((2, 16, 16, width), F32),
            pltpu.VMEM((2, count, width), F32),
            pltpu.VMEM(planes, F32),
            pltpu.VMEM(planes, F32),
            pltpu.SemaphoreType.DMA((5,)),
            pltpu.SemaphoreType.DMA((9,)),
            pltpu.SemaphoreType.DMA((9,)),
            pltpu.SemaphoreType.DMA((96,)),
            pltpu.SemaphoreType.DMA((96,)),
        ],
        compiler_params=pltpu.CompilerParams(collective_id=1, has_side_effects=True, vmem_limit_bytes=66_600_000),
    )(offsets, pattern, sigma_in, hamiltonian, coupling, coulomb)
    spread = (2, 1, 1, width, width)
    return green.reshape(spread), screened.reshape(spread)


def solution(mesh):
    spread = P(None, ("energy", "role"), "block", None, None)
    in_specs = (
        spread,
        P("block", None, None),
        P("block", None, None),
        P("block", ("energy", "role")),
        P(None, "block", None, None),
        P(),
    )
    return jax.shard_map(body, mesh=mesh, in_specs=in_specs, out_specs=(spread, spread), check_vma=False)
```

```python
import functools

import jax
import jax.numpy as jnp
from jax import lax
from jax.experimental import pallas as pl
from jax.experimental.pallas import tpu as pltpu
from jax.sharding import PartitionSpec as P

TILE = 32
ETA = 0.1
CONTACT = 0.5
HIGH = lax.Precision.HIGHEST
F32 = jnp.float32


def dot(a, b):
    return jnp.dot(a, b, precision=HIGH, preferred_element_type=F32)


def row_of(x, k):
    return jnp.broadcast_to(x[k : k + 1, :], (8, 128))


def column_of(x, k):
    return jnp.broadcast_to(x[:, k : k + 1], (8, 128))


def times(a, b):
    return a[0] * b[0] - a[1] * b[1], a[0] * b[1] + a[1] * b[0]


def pair_step(cols, panel, k):
    row = lax.broadcasted_iota(jnp.int32, (8, 128), 0)
    l = k + 1
    at_k, at_l = row == k, row == l
    both = at_k | at_l
    ck, cl = cols[k], cols[l]
    a = row_of(ck[0], k), row_of(ck[1], k)
    b = row_of(cl[0], k), row_of(cl[1], k)
    c = row_of(ck[0], l), row_of(ck[1], l)
    d = row_of(cl[0], l), row_of(cl[1], l)
    ad, bc = times(a, d), times(b, c)
    er, ei = ad[0] - bc[0], ad[1] - bc[1]
    r = 1.0 / (er * er + ei * ei)
    kd, lc = times(ck, d), times(cl, c)
    la, kb = times(cl, a), times(ck, b)
    uk = tuple(jnp.where(at_k, -d[p], jnp.where(at_l, c[p], kd[p] - lc[p])) for p in (0, 1))
    ul = tuple(jnp.where(at_k, b[p], jnp.where(at_l, -a[p], la[p] - kb[p])) for p in (0, 1))
    inv = er * r, -(ei * r)
    tk, tl = times(uk, inv), times(ul, inv)

    def update(z):
        x, y = z
        u = times(tk, (row_of(x, k), row_of(y, k)))
        v = times(tl, (row_of(x, l), row_of(y, l)))
        return jnp.where(both, 0.0, x) - (u[0] + v[0]), jnp.where(both, 0.0, y) - (u[1] + v[1])

    return [z if j <= l else update(z) for j, z in enumerate(cols)], update(panel)


def panels_inverse(chains, base):
    lane = lax.broadcasted_iota(jnp.int32, (8, 128), 1)
    row = lax.broadcasted_iota(jnp.int32, (8, 128), 0)
    chains = [(list(a), list(b)) for a, b in chains]
    total = len(chains[0][0])
    for q in range(4):
        at = base + 8 * q
        inside = (lane >= at) & (lane < at + 8)
        unit = jnp.where(lane - at == row, 1.0, 0.0)
        work = []
        for pr, pi in chains:
            cols = [(column_of(pr[q], at + j), column_of(pi[q], at + j)) for j in range(8)]
            work.append((cols, (jnp.where(inside, unit, pr[q]), jnp.where(inside, 0.0, pi[q]))))
        for k in range(0, 8, 2):
            work = [pair_step(cols, panel, k) for cols, panel in work]
        rows = [[(row_of(n[0], j), row_of(n[1], j)) for j in range(8)] for _, n in work]
        for i in [(q + 1 + i) % total for i in range(total)]:
            if i == q:
                continue
            for (pr, pi), own in zip(chains, rows):
                terms = [times((column_of(pr[i], at + j), column_of(pi[i], at + j)), own[j]) for j in range(8)]
                while len(terms) > 1:
                    pairs = zip(terms[::2], terms[1::2])
                    terms = [(m[0] + n[0], m[1] + n[1]) for m, n in pairs]
                pr[i] = jnp.where(inside, 0.0, pr[i]) - terms[0][0]
                pi[i] = jnp.where(inside, 0.0, pi[i]) - terms[0][1]
        for (pr, pi), (_, n) in zip(chains, work):
            pr[q], pi[q] = n
    return chains


def inverses(matrices):
    lane = lax.broadcasted_iota(jnp.int32, (8, 128), 1)
    state = [[[part[8 * s : 8 * s + 8] for s in range(16)] for part in m] for m in matrices]
    for p in range(4):
        base = 32 * p
        own = [4 * p + i for i in range(4 if p == 3 else 5)]
        others = [s % 16 for s in range(4 * p + len(own), 4 * p + 16)]
        inside = (lane >= base) & (lane < base + 32)
        panels = panels_inverse([([xr[s] for s in own], [xi[s] for s in own]) for xr, xi in state], base)
        following = []
        for (xr, xi), (nr, ni) in zip(state, panels):
            old_r = jnp.concatenate([xr[o] for o in others], 0)
            old_i = jnp.concatenate([xi[o] for o in others], 0)
            left = jnp.concatenate([old_r[:, base : base + 32], old_i[:, base : base + 32]], 1)
            fr, fi = jnp.concatenate(nr[:4], 0), jnp.concatenate(ni[:4], 0)
            right = jnp.concatenate([jnp.concatenate([fr, fi], 1), jnp.concatenate([-fi, fr], 1)], 0)
            change = dot(left, right)
            yr, yi = [None] * 16, [None] * 16
            for t, o in enumerate(others):
                yr[o] = jnp.where(inside, 0.0, xr[o]) - change[8 * t : 8 * t + 8, :128]
                yi[o] = jnp.where(inside, 0.0, xi[o]) - change[8 * t : 8 * t + 8, 128:]
            for t, o in enumerate(own):
                yr[o], yi[o] = nr[t], ni[t]
            following.append((yr, yi))
        state = following
    return [(jnp.concatenate(a, 0), jnp.concatenate(b, 0)) for a, b in state]


def complex_dot(a, b):
    left = jnp.concatenate(a, 1)
    right = jnp.concatenate([jnp.concatenate([b[0], b[1]], 1), jnp.concatenate([-b[1], b[0]], 1)], 0)
    whole = dot(left, right)
    return whole[:, :128], whole[:, 128:]


def real_left(k, g):
    whole = dot(k, jnp.concatenate(g, 1))
    return whole[:, :128], whole[:, 128:]


def real_right(g, k):
    whole = dot(jnp.concatenate(g, 0), k)
    return whole[:128], whole[128:]


def minus(a, b):
    return a[0] - b[0], a[1] - b[1]


def tile_row(tiles_ref, p, i, rows, width):
    lane = lax.broadcasted_iota(jnp.int32, (rows, width), 1)
    strip = jnp.zeros((rows, width), F32)
    for j in range(width // TILE):
        strip = jnp.where((lane >= TILE * j) & (lane < TILE * j + TILE), tiles_ref[p, 0, i, j].astype(F32), strip)
    return strip


def exchange(place, cur, mid, out, send, recv, base):
    slow, fast, row_partner, slow_partner = place
    started = []

    def push(source, target, index, device):
        copy = pltpu.make_async_remote_copy(
            src_ref=source,
            dst_ref=target,
            send_sem=send.at[base + index],
            recv_sem=recv.at[base + index],
            device_id=device,
            device_id_type=pl.DeviceIdType.MESH,
        )
        copy.start()
        return copy

    fasts = sorted(range(1, 16), key=lambda s: -min(s, 16 - s))
    slows = sorted(range(1, 8), key=lambda s: -min(s, 8 - s))
    one, two = [], []
    for s in slows:
        t, device = slow_partner(s)
        two.append(push(cur.at[1, t], mid.at[1, slow], 16 + s, device))
    for s in fasts:
        t, device = row_partner(s)
        one.append(push(cur.at[0, :, t, :], mid.at[0, :, fast, :], s, device))
    mid[0, :, pl.ds(fast, 1), :] = cur[0, :, pl.ds(fast, 1), :]
    mid[1, pl.ds(slow, 1)] = cur[1, pl.ds(slow, 1)]
    for copy in two:
        copy.wait_recv()
    for s in fasts:
        t, device = row_partner(s)
        started.append(push(mid.at[1, :, t, :], out.at[1, :, fast, :], 24 + s, device))
    for copy in one:
        copy.wait_recv()
    for s in slows:
        t, device = slow_partner(s)
        started.append(push(mid.at[0, t], out.at[0, slow], 40 + s, device))
    out[1, :, pl.ds(fast, 1), :] = mid[1, :, pl.ds(fast, 1), :]
    out[0, pl.ds(slow, 1)] = mid[0, pl.ds(slow, 1)]
    for copy in started:
        copy.wait_recv()
    for copy in one + two + started:
        copy.wait_send()


MESH = pl.DeviceIdType.MESH


def build_system(position, tiles_ref, sigma_ref, hamiltonian_ref, coupling_ref, x_ref):
    place = lax.axis_index("energy") * lax.axis_size("role") + lax.axis_index("role")
    width = hamiltonian_ref.shape[-1]
    row = lax.broadcasted_iota(jnp.int32, (width, width), 0)
    column = lax.broadcasted_iota(jnp.int32, (width, width), 1)
    strips = [tile_row(tiles_ref, 0, i, TILE, width) for i in range(width // TILE)]
    masked = hamiltonian_ref[0] * jnp.concatenate(strips, 0)
    onsite = 0.5 * (masked + masked.T)
    groups = lax.axis_size("energy") * lax.axis_size("role")
    energy = -3.0 + 6.0 * place.astype(F32) / groups
    k = coupling_ref[0]
    diagonal = row == column
    real = jnp.where(diagonal, energy, 0.0) - onsite - sigma_ref[0, 0, 0]
    bare = jnp.where(diagonal, ETA, 0.0) - sigma_ref[1, 0, 0]
    imag = bare + jnp.where(position == 3, CONTACT * dot(k.T, k), 0.0)
    x_ref[pl.ds(position, 1)] = jnp.stack([real, imag])[None]


def solve(position, x_ref, k_ref, couplings_arrived):
    forward = position >= 2
    first = jnp.where(forward, 0, 3)
    second = jnp.where(forward, 1, 2)
    third = jnp.where(forward, 2, 1)
    fourth = jnp.where(forward, 3, 0)

    def both(index, plain):
        k = k_ref[index]
        kt = k.T
        return jnp.where(plain, k, kt), jnp.where(plain, kt, k)

    ga, gd = inverses([(x_ref[first, 0], x_ref[first, 1]), (x_ref[fourth, 0], x_ref[fourth, 1])])
    couplings_arrived()
    k1, k1t = both(jnp.where(forward, 0, 2), forward)
    k2, k2t = both(1, forward)
    k3, k3t = both(jnp.where(forward, 2, 0), jnp.logical_not(forward))
    sb = minus((x_ref[second, 0], x_ref[second, 1]), real_right(real_left(k1t, ga), k1))
    (gb,) = inverses([sb])
    gd_k3 = real_right(gd, k3)
    k3t_gd = real_left(k3t, gd)
    sc = minus((x_ref[third, 0], x_ref[third, 1]), real_right(k3t_gd, k3))
    sc = minus(sc, real_right(real_left(k2t, gb), k2))
    (gc,) = inverses([sc])
    back = complex_dot(complex_dot(gd_k3, gc), k3t_gd)
    inner = (position == 1) | (position == 2)
    return [jnp.where(inner, gc[part], gd[part] + back[part]) for part in (0, 1)]


def whole_kernel(
    count,
    offsets_ref,
    tiles,
    sigma,
    hamiltonian,
    coupling,
    coulomb,
    green_ref,
    o_ref,
    tiles_ref,
    sigma_ref,
    hamiltonian_ref,
    coulomb_ref,
    x_ref,
    k_ref,
    held,
    mid,
    padded,
    polar,
    done,
    mid_back,
    local,
    ring_send,
    ring_recv,
    send,
    recv,
):
    energies = 128
    factor = 6.0 / energies / (2.0 * 3.141592653589793)
    position = lax.axis_index("block")
    e, c = lax.axis_index("energy"), lax.axis_index("role")
    slow, z = e // 8, lax.rem(e, 8)
    fast = 2 * z + c
    right, opposite, left = [lax.rem(position + s, 4) for s in (1, 2, 3)]
    pairs = (
        (coupling, k_ref.at[pl.ds(position, 1)]),
        (tiles, tiles_ref),
        (sigma, sigma_ref),
        (hamiltonian, hamiltonian_ref),
        (coulomb, coulomb_ref),
    )
    loads = [pltpu.make_async_copy(source, target, local.at[i]) for i, (source, target) in enumerate(pairs)]
    for load in loads:
        load.start()

    def row_partner(s):
        t = lax.rem(fast + s, 16)
        return t, {"energy": slow * 8 + t // 2, "role": lax.rem(t, 2)}

    def slow_partner(s):
        t = lax.rem(slow + s, 8)
        return t, {"energy": t * 8 + z, "role": c}

    place = slow, fast, row_partner, slow_partner
    barrier = pltpu.get_barrier_semaphore()
    for partner, others in ((row_partner, 16), (slow_partner, 8)):
        for s in range(1, others):
            pl.semaphore_signal(barrier, inc=1, device_id=partner(s)[1], device_id_type=MESH)
    for block in (right, opposite, left):
        pl.semaphore_signal(barrier, inc=1, device_id={"block": block}, device_id_type=MESH)
    padded[:, :8] = jnp.zeros((2, 8, 16, 128), F32)
    for load in loads:
        load.wait()
    build_system(position, tiles_ref, sigma_ref, hamiltonian_ref, k_ref.at[pl.ds(position, 1)], x_ref)
    pl.semaphore_wait(barrier, 25)

    def push(ref, index, block):
        return pltpu.make_async_remote_copy(
            src_ref=ref,
            dst_ref=ref,
            send_sem=ring_send.at[index],
            recv_sem=ring_recv.at[index],
            device_id={"block": block},
            device_id_type=MESH,
        )

    def system(owner, lower):
        return x_ref.at[owner, :, pl.ds(64 * lower, 64), :]

    early = [push(system(position, 0), 0, right), push(system(position, 1), 1, left)]
    late = [push(system(position, 1), 2, right), push(system(position, 0), 3, left)]
    onward = [push(system(left, 0), 4, right), push(system(right, 1), 5, left)]
    couplings = [push(k_ref.at[position], 6 + i, block) for i, block in enumerate((right, opposite, left))]
    for copy in early + late:
        copy.start()
    for copy, following in zip(early, onward):
        copy.wait_recv()
        following.start()
    for copy in couplings:
        copy.start()
    for copy in late + onward:
        copy.wait_recv()

    def couplings_arrived():
        for copy in couplings:
            copy.wait_recv()
        for copy in early + late + onward + couplings:
            copy.wait_send()

    green = solve(position, x_ref, k_ref, couplings_arrived)
    for part in (0, 1):
        held[part] = green[part].reshape(8, 16, 128)
        green_ref[part] = green[part]
    exchange(place, held, mid, padded.at[:, 8:], send, recv, 0)
    flat = padded.reshape(2, 2 * energies, 128)
    result = done.reshape(2, energies, 128)

    def polarize(w, carry):
        start = energies - offsets_ref[w]
        mr, mi = flat[0, pl.ds(start, energies), :], flat[1, pl.ds(start, energies), :]
        vr, vi = flat[0, energies:, :], flat[1, energies:, :]
        polar[0, pl.ds(w, 1), :] = factor * jnp.sum(vr * mr - vi * mi, axis=0, keepdims=True)
        polar[1, pl.ds(w, 1), :] = factor * jnp.sum(vr * mi + vi * mr, axis=0, keepdims=True)
        return carry

    lax.fori_loop(0, count, polarize, 0, unroll=4)
    weight = coulomb_ref[...] * tile_row(tiles_ref, 1, (2 * e + c) // TILE, 1, 128)
    scale = weight * weight * (1.0 / count)
    rows = 64
    for n in range(0, energies, rows):

        def interact(w, total):
            start = energies - offsets_ref[w] + n
            mr, mi = flat[0, pl.ds(start, rows), :], flat[1, pl.ds(start, rows), :]
            pr, pi = polar[0, pl.ds(w, 1), :], polar[1, pl.ds(w, 1), :]
            return total[0] + (mr * pr - mi * pi), total[1] + (mr * pi + mi * pr)

        zero = jnp.zeros((rows, 128), F32)
        tr, ti = lax.fori_loop(0, count, interact, (zero, zero), unroll=4)
        result[0, n : n + rows] = tr * scale
        result[1, n : n + rows] = ti * scale
    exchange(place, done, mid_back, o_ref, send, recv, 48)


def in_vmem():
    return pl.BlockSpec(memory_space=pltpu.VMEM)


def in_smem():
    return pl.BlockSpec(memory_space=pltpu.SMEM)


def body(sigma_in, hamiltonian, coupling, coulomb, pattern, offsets):
    width = hamiltonian.shape[-1]
    count = offsets.shape[0]
    planes = (2, 8, 16, width)
    green, screened = pl.pallas_call(
        functools.partial(whole_kernel, count),
        out_shape=[jax.ShapeDtypeStruct((2, width, width), F32), jax.ShapeDtypeStruct(planes, F32)],
        in_specs=[in_smem()] + [pl.BlockSpec(memory_space=pl.ANY)] * 5,
        out_specs=[in_vmem()] * 2,
        scratch_shapes=[
            pltpu.SMEM(pattern.shape, pattern.dtype),
            pltpu.VMEM(sigma_in.shape, F32),
            pltpu.VMEM(hamiltonian.shape, F32),
            pltpu.VMEM(coulomb.shape, F32),
            pltpu.VMEM((4, 2, width, width), F32),
            pltpu.VMEM((4, width, width), F32),
            pltpu.VMEM(planes, F32),
            pltpu.VMEM(planes, F32),
            pltpu.VMEM((2, 16, 16, width), F32),
            pltpu.VMEM((2, count, width), F32),
            pltpu.VMEM(planes, F32),
            pltpu.VMEM(planes, F32),
            pltpu.SemaphoreType.DMA((5,)),
            pltpu.SemaphoreType.DMA((9,)),
            pltpu.SemaphoreType.DMA((9,)),
            pltpu.SemaphoreType.DMA((96,)),
            pltpu.SemaphoreType.DMA((96,)),
        ],
        compiler_params=pltpu.CompilerParams(collective_id=1, has_side_effects=True, vmem_limit_bytes=66_600_000),
    )(offsets, pattern, sigma_in, hamiltonian, coupling, coulomb)
    spread = (2, 1, 1, width, width)
    return green.reshape(spread), screened.reshape(spread)


def solution(mesh):
    spread = P(None, ("energy", "role"), "block", None, None)
    in_specs = (
        spread,
        P("block", None, None),
        P("block", None, None),
        P("block", ("energy", "role")),
        P(None, "block", None, None),
        P(),
    )
    return jax.shard_map(body, mesh=mesh, in_specs=in_specs, out_specs=(spread, spread), check_vma=False)
```
